32 devices in a mesh: row: 8 (over z, y), col: 4 (over x, core).
Axes of the slice: x: 2, y: 2, z: 4, core: 2. Of those that a mesh axis runs over, the one named last changes fastest.
Arguments:
- matrix_tiles: float32 [8, 4, 16, 256, 256], P('row', 'col'), may hold values from -0.3125 to 0.3125
- tile_slot: int32 [8, 4, 16], P('row', 'col'), may hold values from 0 to 2047, as said below
- cost_vector: float32 [512, 256], P('col'), may hold values from -24 to 24
- lower_bound: float32 [512, 256], P('col'), may hold values from -4 to 4
- bound_width: float32 [512, 256], P('col'), may hold values from 0.5 to 4
- variable_kind: int32 [512, 256], P('col'), may hold values from 0 to 2
- right_side: float32 [128, 256], P('row'), may hold values from -24 to 24
- row_kind: int32 [128, 256], P('row'), may hold values from 0 to 1
- primal_start: float32 [512, 256], P('col'), may hold values from -6 to 6
- dual_start: float32 [128, 256], P('row'), may hold values from -3 to 3
- primal_weight: float32 [], replicated, may hold values from 0.7 to 1.4
- step_start: float32 [], replicated, may hold values from 1 to 2
Outputs:
- primal: float32 [512, 256], P('col')
- dual: float32 [128, 256], P('row')
The draws below stay inside these ranges and needn't reach their ends.
Inputs may be any that keep to these rules, and one draw needn't show every extreme that they name: `tile_slot`: within each block [r, c] the 16 tiles lie in different column tiles. Split a block's 128 column tiles into runs of 16 in a row: no run holds more than 2 of the block's tiles.
All inputs are finite; a program needn't handle non-finite values.
Results may differ from the reference program's by a relative error of at most 0.00026.
Values sent between devices are 32-bit elements; how exact they have to be, the bound alone decides.
No kernel may reach another device: no remote copies, remote signals or barrier semaphores. Data moves between devices by JAX's collectives and lax.ppermute only.
A program may use at most 64 MiB of HBM per device.

```python
import math
import jax
import jax.numpy as jnp
from jax import lax

TILE = 256
RT_DEV = 16
CT_DEV = 128
TILES_DEV = 16
ITERS = 4
RTILES = 128
CTILES = 512
N_ROW = 8
N_COL = 4


def draw_tile_slot(key, part):
    keys = jax.random.split(key, N_ROW * N_COL)
    share = CT_DEV // N_ROW

    def one_block(block_key):
        key_share, key_offset, key_row = jax.random.split(block_key, 3)
        order = jax.random.permutation(key_share, N_ROW).astype(jnp.int32)
        offsets = jax.random.randint(key_offset, (N_ROW,), 0, share).astype(jnp.int32)
        counter = jnp.arange(TILES_DEV, dtype=jnp.int32)
        which = order[counter % N_ROW]
        inside = (counter // N_ROW + offsets[counter % N_ROW]) % share
        rows = jax.random.randint(key_row, (TILES_DEV,), 0, RT_DEV).astype(jnp.int32)
        return rows * CT_DEV + which * share + inside
    return jax.vmap(one_block)(keys).reshape(N_ROW, N_COL, TILES_DEV).astype(jnp.int32)


def rising_field(key, count):
    ramp = jnp.arange(count, dtype=jnp.float32) / jnp.float32(max(count - 1, 1))
    values = jnp.clip(jax.random.normal(key, (count, TILE), jnp.float32), -6.0, 6.0)
    scale = 1.0 + 2.0 * ramp
    return (values * scale[:, None]).astype(jnp.float32)


def draw_cost_vector(key, part):
    return rising_field(jax.random.fold_in(key, 11), CTILES)


def draw_right_side(key, part):
    return rising_field(jax.random.fold_in(key, 23), RTILES)


def touch_ends(result, stream_key, low, high):
    dims = result.shape
    index_at = [jax.random.randint(jax.random.fold_in(stream_key, axis), (), 0, dims[axis]) for axis in range(len(dims))]
    result = result.at[tuple(index_at)].set(low)
    longest = dims.index(max(dims))
    index_at[longest] = (index_at[longest] + 1) % dims[longest]
    return result.at[tuple(index_at)].set(high)


def level_of(own_key, dims, cuts, smallest, high):
    factor_of = 1.0
    for position, blocks in cuts:
        steps = jax.random.uniform(jax.random.fold_in(jax.random.fold_in(own_key, 6), position), (blocks,), jnp.float32, smallest / len(cuts), high / len(cuts))
        factor_of = factor_of * jnp.repeat(jnp.exp(steps), dims[position] // blocks).reshape((-1,) + (1,) * (len(dims) - 1 - position))
    return factor_of


def normal_values(key, dims, spread, most, shards=(), kind=jnp.bfloat16):
    array = jax.random.normal(key, dims, jnp.float32) * spread
    if len(shards) > 0:
        array = level_of(key, dims, shards, -0.22, 0.18) * array
    return jnp.clip(array, min=-most, max=most).astype(kind)


def setup_inputs(seed: int = 0) -> dict:
    key_of = jax.random.split(jax.random.key(seed), 13)
    matrix_tiles = normal_values(key_of[0], (N_ROW, N_COL, TILES_DEV, TILE, TILE), ((8 * TILE) ** -0.5), 0.3125, ((0, 8), (1, 4)), jnp.float32)
    tile_slot = draw_tile_slot(jax.random.fold_in(key_of[12], 71), 0)
    cost_vector = draw_cost_vector(jax.random.fold_in(key_of[12], 71), 0)
    lower_bound = normal_values(key_of[3], (CTILES, TILE), 1.0, 4.0, ((0, 4),), jnp.float32)
    bound_width = jnp.clip(jnp.exp(math.log(4.0) - 2.0794415 * jax.random.uniform(key_of[4], (CTILES, TILE), jnp.float32) ** level_of(key_of[4], (CTILES, TILE), ((0, 4),), -0.2, 0.2)), 0.5, 4.0)
    variable_kind = touch_ends(jax.random.randint(key_of[5], (CTILES, TILE), 0, 3), jax.random.fold_in(key_of[5], 1), 0, 2).astype(jnp.int32)
    right_side = draw_right_side(jax.random.fold_in(key_of[12], 71), 0)
    row_kind = touch_ends(jax.random.randint(key_of[7], (RTILES, TILE), 0, 2), jax.random.fold_in(key_of[7], 1), 0, 1).astype(jnp.int32)
    primal_start = normal_values(key_of[8], (CTILES, TILE), 1.0, 6.0, ((0, 4),), jnp.float32)
    dual_start = normal_values(key_of[9], (RTILES, TILE), 0.5, 3.0, ((0, 8),), jnp.float32)
    primal_weight = jnp.clip(jnp.exp(jax.random.uniform(key_of[10], (), jnp.float32, math.log(0.7), math.log(1.4))), 0.7, 1.4)
    step_start = jnp.clip(jnp.exp(jax.random.uniform(key_of[11], (), jnp.float32, math.log(1.0), math.log(2.0))), 1.0, 2.0)
    return dict(matrix_tiles=matrix_tiles, tile_slot=tile_slot, cost_vector=cost_vector, lower_bound=lower_bound, bound_width=bound_width, variable_kind=variable_kind, right_side=right_side, row_kind=row_kind, primal_start=primal_start, dual_start=dual_start, primal_weight=primal_weight, step_start=step_start)


highest = lax.Precision.HIGHEST


def apply_matrix(matrix_tiles, tile_slot, vector):
    col_of = tile_slot % CT_DEV
    row_of = tile_slot // CT_DEV
    blocks = vector.reshape(N_COL, CT_DEV, TILE)
    picked = blocks[jnp.arange(N_COL, dtype=jnp.int32)[None, :, None], col_of]
    product = jnp.einsum("rctij,rctj->rcti", matrix_tiles, picked, precision=highest)
    onehot = (row_of[..., None] == jnp.arange(RT_DEV, dtype=jnp.int32)).astype(jnp.float32)
    summed = jnp.einsum("rctk,rcti->rki", onehot, product, precision=highest)
    return summed.reshape(N_ROW * RT_DEV, TILE)


def apply_transpose(matrix_tiles, tile_slot, vector):
    col_of = tile_slot % CT_DEV
    row_of = tile_slot // CT_DEV
    blocks = vector.reshape(N_ROW, RT_DEV, TILE)
    picked = blocks[jnp.arange(N_ROW, dtype=jnp.int32)[:, None, None], row_of]
    product = jnp.einsum("rctij,rcti->rctj", matrix_tiles, picked, precision=highest)
    onehot = (col_of[..., None] == jnp.arange(CT_DEV, dtype=jnp.int32)).astype(jnp.float32)
    summed = jnp.einsum("rctk,rctj->ckj", onehot, product, precision=highest)
    return summed.reshape(N_COL * CT_DEV, TILE)


def project_primal(values, lower_bound, bound_width, variable_kind):
    lifted = jnp.where(variable_kind >= 1, jnp.maximum(values, lower_bound), values)
    return jnp.where(variable_kind == 2, jnp.minimum(lifted, lower_bound + bound_width), lifted)


def project_dual(values, row_kind):
    return jnp.where(row_kind == 1, jnp.maximum(values, 0.0), values)


def next_step(cross, dual_square, primal_square, weight, step_size, iteration):
    movement = 0.5 * weight * primal_square + 0.5 * dual_square / weight
    count = iteration + 11.0
    return movement / jnp.maximum(jnp.abs(cross) / (1.0 - count ** -0.3), movement / ((1.0 + count ** -0.6) * step_size))


def reference(matrix_tiles, tile_slot, cost_vector, lower_bound, bound_width, variable_kind, right_side, row_kind, primal_start, dual_start, primal_weight, step_start):
    primal, dual = primal_start, dual_start
    step_size = step_start
    image = apply_matrix(matrix_tiles, tile_slot, primal)
    gradient = apply_transpose(matrix_tiles, tile_slot, dual)
    for iteration in range(ITERS):
        primal_next = project_primal(primal - (step_size / primal_weight) * (cost_vector - gradient), lower_bound, bound_width, variable_kind)
        image_next = apply_matrix(matrix_tiles, tile_slot, primal_next)
        dual_next = project_dual(dual + (step_size * primal_weight) * (right_side - 2.0 * image_next + image), row_kind)
        if iteration + 1 < ITERS:
            gradient = apply_transpose(matrix_tiles, tile_slot, dual_next)
            change_dual = dual_next - dual
            change_primal = primal_next - primal
            cross = jnp.sum(change_dual * (image_next - image))
            dual_square = jnp.sum(change_dual * change_dual)
            primal_square = jnp.sum(change_primal * change_primal)
            step_size = next_step(cross, dual_square, primal_square, primal_weight, step_size, iteration)
        primal, dual, image = primal_next, dual_next, image_next
    return primal, dual
```

```python
import functools

import jax
import jax.numpy as jnp
from jax import lax
from jax.experimental import pallas as pl
from jax.experimental.pallas import tpu as pltpu
from jax.sharding import PartitionSpec as P

ITERS = 4

highest = lax.Precision.HIGHEST


def square_sum(values):
    return jnp.sum(jnp.sum(values, axis=0, keepdims=True), axis=1, keepdims=True)


def columns_of(rows):
    count, width = rows.shape
    padded = jnp.concatenate([rows, jnp.zeros((128 - count, width), rows.dtype)], axis=0)
    return padded.T


def forward(tiles_ref, slots_ref, vector_ref, row_tiles, col_tiles):
    tile_count, height, width = tiles_ref.shape
    lane = lax.broadcasted_iota(jnp.int32, (height, 128), 1)

    def step(t, total):
        slot = slots_ref[t]
        picked = vector_ref[pl.ds(slot % col_tiles, 1), :]
        product = jnp.sum(tiles_ref[t] * picked, axis=1, keepdims=True)
        return total + jnp.where(lane == slot // col_tiles, product, 0.0)

    total = lax.fori_loop(0, tile_count, step, jnp.zeros((height, 128), jnp.float32), unroll=2)
    return total.T[:row_tiles]


def backward(tiles_ref, slots_ref, rows, out_ref, col_tiles):
    tile_count, height, width = tiles_ref.shape
    columns = columns_of(rows)
    lane = lax.broadcasted_iota(jnp.int32, columns.shape, 1)

    def step(t, carry):
        slot = slots_ref[t]
        mine = jnp.where(lane == slot // col_tiles, columns, 0.0)
        picked = jnp.sum(mine, axis=1, keepdims=True)
        out_ref[pl.ds(t, 1), :width] = jnp.sum(tiles_ref[t] * picked, axis=0, keepdims=True)
        return carry

    lax.fori_loop(0, tile_count, step, 0, unroll=2)


def start_kernel(slots_ref, tiles_ref, dual_ref, out_ref, *, col_tiles):
    tile_count, height, width = tiles_ref.shape
    lane = lax.broadcasted_iota(jnp.int32, (1, out_ref.shape[1] - width), 1)
    for t in range(tile_count):
        column = slots_ref[t] % col_tiles
        out_ref[t : t + 1, width:] = jnp.full(lane.shape, column, jnp.int32).astype(jnp.float32)
    backward(tiles_ref, slots_ref, dual_ref[...], out_ref, col_tiles)


def image_kernel(slots_ref, tiles_ref, vector_ref, out_ref):
    out_ref[...] = forward(
        tiles_ref, slots_ref, vector_ref, out_ref.shape[0], vector_ref.shape[0]
    )


def primal_kernel(*refs, iteration, part_count):
    refs = list(refs)
    slots_ref, place_ref, scalars_ref = refs[:3]
    part_refs = refs[3 : 3 + part_count]
    refs = refs[3 + part_count :]
    tiles_ref, primal_ref, cost_ref, lower_ref, width_ref, kind_ref = refs[:6]
    refs = refs[6:]
    if iteration > 0:
        hot_ref, step_ref, moved_ref = refs[:3]
        refs = refs[3:]
    out_ref, primal_out, step_out = refs[:3]
    refs = refs[3:]
    if iteration == 0:
        hot_ref = refs[0]
        refs = refs[1:]
    gather_ref = refs[0]

    width = primal_ref.shape[1]
    col_tiles = primal_ref.shape[0]
    row_tiles = out_ref.shape[0]
    part_rows = part_refs[0].shape[0]
    for k in range(part_count):
        gather_ref[pl.ds(pl.multiple_of(place_ref[k] * part_rows, 8), part_rows), :] = part_refs[k][...]
    weight = scalars_ref[0]
    if iteration == 0:
        number = lax.broadcasted_iota(jnp.int32, hot_ref.shape, 1).astype(jnp.float32)
        hot_ref[...] = (gather_ref[:, width:] == number).astype(jnp.float32)
        step_size = jnp.full((1, 1), scalars_ref[1], jnp.float32)
    else:
        tile_count = tiles_ref.shape[0]
        sources = gather_ref.shape[0] // tile_count
        sums = gather_ref[:tile_count, width:]
        for r in range(1, sources):
            sums = sums + gather_ref[r * tile_count : (r + 1) * tile_count, width:]
        cross = sums[0:1, 0:1]
        dual_square = sums[1:2, 0:1]
        primal_square = moved_ref[0:1, 0:1]
        before = step_ref[0:1, 0:1]
        movement = 0.5 * weight * primal_square + 0.5 * dual_square / weight
        count = iteration - 1 + 11.0
        step_size = movement / jnp.maximum(
            jnp.abs(cross) / (1.0 - count ** (-0.3)),
            movement / ((1.0 + count ** (-0.6)) * before),
        )
    step_out[...] = jnp.broadcast_to(step_size, step_out.shape)
    gradient = lax.dot_general(
        hot_ref[...],
        gather_ref[:, :width],
        (((0,), (0,)), ((), ())),
        precision=highest,
        preferred_element_type=jnp.float32,
    )
    primal = primal_ref[...]
    kind = kind_ref[...]
    lower = lower_ref[...]
    values = primal - (step_size / weight) * (cost_ref[...] - gradient)
    lifted = jnp.where(kind >= 1, jnp.maximum(values, lower), values)
    primal_next = jnp.where(kind == 2, jnp.minimum(lifted, lower + width_ref[...]), lifted)
    primal_out[...] = primal_next
    change = primal_next - primal
    out_ref[:, width:] = jnp.broadcast_to(
        square_sum(change * change), (row_tiles, out_ref.shape[1] - width)
    )
    out_ref[:, :width] = forward(tiles_ref, slots_ref, primal_out, row_tiles, col_tiles)


def dual_kernel(*refs, last, first, part_count, col_tiles):
    refs = list(refs)
    slots_ref, scalars_ref = refs[:2]
    part_refs = refs[2 : 2 + part_count]
    refs = refs[2 + part_count :]
    if first:
        start_refs = refs[:part_count]
        refs = refs[part_count:]
    else:
        image_ref = refs[0]
        refs = refs[1:]
    tiles_ref, step_ref, dual_ref, side_ref, kind_ref, dual_out = refs[:6]
    refs = refs[6:]

    def combined(those):
        values = [ref[...] for ref in those]
        while len(values) > 1:
            values = [values[i] + values[i + 1] for i in range(0, len(values), 2)]
        return values[0]

    width = dual_ref.shape[1]
    weight = scalars_ref[0]
    total = combined(part_refs)
    image_next = total[:, :width]
    image = combined(start_refs) if first else image_ref[...]
    dual = dual_ref[...]
    step_size = step_ref[0:1, 0:1]
    values = dual + (step_size * weight) * (side_ref[...] - 2.0 * image_next + image)
    dual_next = jnp.where(kind_ref[...] == 1, jnp.maximum(values, 0.0), values)
    dual_out[...] = dual_next
    if last:
        return
    out_ref, image_out, moved_out = refs[:3]
    image_out[...] = image_next
    moved_out[...] = total[:8, width : width + 128]
    change = dual_next - dual
    cross = square_sum(change * (image_next - image))
    dual_square = square_sum(change * change)
    extra = (out_ref.shape[0], out_ref.shape[1] - width)
    which = lax.broadcasted_iota(jnp.int32, extra, 0)
    out_ref[:, width:] = jnp.where(
        which == 0, cross, jnp.where(which == 1, dual_square, 0.0)
    )
    backward(tiles_ref, slots_ref, dual_next, out_ref, col_tiles)


def call(kernel, outs, inputs, scratch=(), spaces=None):
    spaces = spaces or {}
    specs = [
        pl.BlockSpec(memory_space=spaces.get(i, pltpu.VMEM)) for i in range(len(inputs))
    ]
    return pl.pallas_call(
        kernel,
        out_shape=outs,
        in_specs=specs,
        out_specs=[pl.BlockSpec(memory_space=pltpu.VMEM) for _ in outs],
        scratch_shapes=scratch,
        compiler_params=pltpu.CompilerParams(vmem_limit_bytes=32 * 1024 * 1024),
    )(*inputs)


def exchange(values, axis, size):
    others = [
        lax.ppermute(values, axis, [(i, i ^ k) for i in range(size)]) for k in range(1, size)
    ]
    return [values] + others


def gather_rows(values, size):
    copies = jnp.broadcast_to(values[None], (size,) + values.shape)
    arrived = lax.all_to_all(copies, "row", split_axis=0, concat_axis=0)
    return [arrived.reshape(-1, values.shape[-1])], jnp.zeros((1,), jnp.int32)


def shards(
    matrix_tiles,
    tile_slot,
    cost_vector,
    lower_bound,
    bound_width,
    variable_kind,
    right_side,
    row_kind,
    primal_start,
    dual_start,
    primal_weight,
    step_start,
):
    tile_set = matrix_tiles[0, 0]
    slots = tile_slot[0, 0]
    row_tiles, width = right_side.shape
    col_tiles = cost_vector.shape[0]
    tile_count = slots.shape[0]
    row_count = lax.axis_size("row")
    col_count = lax.axis_size("col")
    scalars = jnp.stack([primal_weight, step_start])
    f32 = jnp.float32
    smem = pltpu.SMEM
    sent_shape = (tile_count, width + col_tiles)
    image_shape = (row_tiles, width + 128)

    tiles = tile_set
    (sent,) = call(
        functools.partial(start_kernel, col_tiles=col_tiles),
        [jax.ShapeDtypeStruct(sent_shape, f32)],
        [slots, tiles, dual_start],
        spaces={0: smem},
    )
    (image_start,) = call(
        image_kernel,
        [jax.ShapeDtypeStruct((row_tiles, width), f32)],
        [slots, tiles, primal_start],
        spaces={0: smem},
    )
    start_parts = exchange(image_start, "col", col_count)
    primal, dual = primal_start, dual_start
    hot = step_size = moved = image = None
    for iteration in range(ITERS):
        parts, places = gather_rows(sent, row_count)
        first, last = iteration == 0, iteration + 1 == ITERS
        sources = row_count * tile_count
        outs = [
            jax.ShapeDtypeStruct(image_shape, f32),
            jax.ShapeDtypeStruct(primal.shape, f32),
            jax.ShapeDtypeStruct((8, 128), f32),
        ]
        inputs = [slots, places, scalars, *parts, tiles, primal]
        inputs += [cost_vector, lower_bound, bound_width, variable_kind]
        if first:
            outs.append(jax.ShapeDtypeStruct((sources, col_tiles), f32))
        else:
            inputs += [hot, step_size, moved]
        results = call(
            functools.partial(primal_kernel, iteration=iteration, part_count=len(parts)),
            outs,
            inputs,
            scratch=[pltpu.VMEM((sources, width + col_tiles), f32)],
            spaces={0: smem, 1: smem, 2: smem},
        )
        image_part, primal, step_size = results[:3]
        if first:
            hot = results[3]
        parts = exchange(image_part, "col", col_count)
        outs = [jax.ShapeDtypeStruct(dual.shape, f32)]
        if not last:
            outs += [
                jax.ShapeDtypeStruct(sent_shape, f32),
                jax.ShapeDtypeStruct(dual.shape, f32),
                jax.ShapeDtypeStruct((8, 128), f32),
            ]
        inputs = [slots, scalars, *parts]
        inputs += start_parts if first else [image]
        inputs += [tiles, step_size, dual, right_side, row_kind]
        results = call(
            functools.partial(
                dual_kernel, last=last, first=first, part_count=len(parts), col_tiles=col_tiles
            ),
            outs,
            inputs,
            spaces={0: smem, 1: smem},
        )
        dual = results[0]
        if not last:
            sent, image, moved = results[1:]
    return (primal, dual)


def solution(mesh):
    return jax.shard_map(
        shards,
        mesh=mesh,
        in_specs=(
            P("row", "col", None, None, None),
            P("row", "col", None),
            P("col", None),
            P("col", None),
            P("col", None),
            P("col", None),
            P("row", None),
            P("row", None),
            P("col", None),
            P("row", None),
            P(),
            P(),
        ),
        out_specs=(P("col", None), P("row", None)),
        check_vma=False,
    )
```

```python
import functools

import jax
import jax.numpy as jnp
from jax import lax
from jax.experimental import pallas as pl
from jax.experimental.pallas import tpu as pltpu
from jax.sharding import PartitionSpec as P

ITERS = 4
LANES = 128

highest = lax.Precision.HIGHEST


def square_sum(values):
    return jnp.sum(jnp.sum(values, axis=0, keepdims=True), axis=1, keepdims=True)


def columns_of(rows):
    count, width = rows.shape
    padded = jnp.concatenate([rows, jnp.zeros((128 - count, width), rows.dtype)], axis=0)
    return padded.T


def forward(tiles_ref, slots_ref, vector_ref, row_tiles, col_tiles):
    tile_count, height, width = tiles_ref.shape
    lane = lax.broadcasted_iota(jnp.int32, (height, 128), 1)

    def step(t, total):
        slot = slots_ref[t]
        picked = vector_ref[pl.ds(slot % col_tiles, 1), :]
        product = jnp.sum(tiles_ref[t] * picked, axis=1, keepdims=True)
        return total + jnp.where(lane == slot // col_tiles, product, 0.0)

    total = lax.fori_loop(0, tile_count, step, jnp.zeros((height, 128), jnp.float32), unroll=2)
    return total.T[:row_tiles]


def backward(tiles_ref, slots_ref, rows, out_ref, col_tiles):
    tile_count, height, width = tiles_ref.shape
    columns = columns_of(rows)
    lane = lax.broadcasted_iota(jnp.int32, columns.shape, 1)
    halves = width // LANES

    def step(t, carry):
        slot = slots_ref[t]
        mine = jnp.where(lane == slot // col_tiles, columns, 0.0)
        picked = jnp.sum(mine, axis=1, keepdims=True)
        product = jnp.sum(tiles_ref[t] * picked, axis=0, keepdims=True)
        for h in range(halves):
            out_ref[pl.ds(h * tile_count + t, 1), :] = product[:, h * LANES : (h + 1) * LANES]
        return carry

    lax.fori_loop(0, tile_count, step, 0, unroll=2)


def pack(out_ref, values, start=0):
    count, width = values.shape
    for h in range(width // LANES):
        block = values[:, h * LANES : (h + 1) * LANES]
        out_ref[start + h * count : start + (h + 1) * count, :] = block


def unpack(values, count, width, start=0):
    blocks = [
        values[start + h * count : start + (h + 1) * count] for h in range(width // LANES)
    ]
    return jnp.concatenate(blocks, axis=1)


def start_kernel(slots_ref, tiles_ref, dual_ref, out_ref, *, col_tiles):
    tile_count, height, width = tiles_ref.shape
    meta = tile_count * (width // LANES)
    for t in range(tile_count):
        column = slots_ref[t] % col_tiles
        out_ref[meta + t : meta + t + 1, :] = jnp.full((1, LANES), column, jnp.int32).astype(
            jnp.float32
        )
    backward(tiles_ref, slots_ref, dual_ref[...], out_ref, col_tiles)


def primal_kernel(*refs, iteration, row_tiles):
    slots_ref, scalars_ref, arrived_ref = refs[:3]
    tiles_ref, primal_ref, cost_ref, lower_ref, width_ref, kind_ref = refs[3:9]
    refs = refs[9:]
    if iteration > 0:
        hot_ref, step_ref, moved_ref = refs[:3]
        refs = refs[3:]
    out_ref, primal_out, step_out = refs[:3]
    refs = refs[3:]
    if iteration == 0:
        hot_ref = refs[0]
        refs = refs[1:]
    gather_ref = refs[0]

    col_tiles, width = primal_ref.shape
    tile_count = tiles_ref.shape[0]
    sources = arrived_ref.shape[0]
    halves = width // LANES
    meta = tile_count * halves
    for r in range(sources):
        for h in range(halves):
            gather_ref[r * tile_count : (r + 1) * tile_count, h * LANES : (h + 1) * LANES] = (
                arrived_ref[r, h * tile_count : (h + 1) * tile_count, :]
            )
    weight = scalars_ref[0:1, 0:1]
    if iteration == 0:
        number = lax.broadcasted_iota(jnp.int32, (tile_count, col_tiles), 1).astype(jnp.float32)
        for r in range(sources):
            column = arrived_ref[r, meta : meta + tile_count, :]
            hot_ref[r * tile_count : (r + 1) * tile_count, :] = (
                column[:, 0:1] == number
            ).astype(jnp.float32)
        step_size = scalars_ref[1:2, 0:1]
    else:
        sums = arrived_ref[0, meta : meta + 8, :]
        for r in range(1, sources):
            sums = sums + arrived_ref[r, meta : meta + 8, :]
        cross = sums[0:1, 0:1]
        dual_square = sums[1:2, 0:1]
        primal_square = moved_ref[0:1, 0:1]
        before = step_ref[0:1, 0:1]
        movement = 0.5 * weight * primal_square + 0.5 * dual_square / weight
        count = iteration - 1 + 11.0
        step_size = movement / jnp.maximum(
            jnp.abs(cross) / (1.0 - count ** (-0.3)),
            movement / ((1.0 + count ** (-0.6)) * before),
        )
    step_out[...] = jnp.broadcast_to(step_size, step_out.shape)
    gradient = lax.dot_general(
        hot_ref[...],
        gather_ref[...],
        (((0,), (0,)), ((), ())),
        precision=highest,
        preferred_element_type=jnp.float32,
    )
    primal = primal_ref[...]
    kind = kind_ref[...]
    lower = lower_ref[...]
    values = primal - (step_size / weight) * (cost_ref[...] - gradient)
    lifted = jnp.where(kind >= 1, jnp.maximum(values, lower), values)
    primal_next = jnp.where(kind == 2, jnp.minimum(lifted, lower + width_ref[...]), lifted)
    primal_out[...] = primal_next
    change = primal_next - primal
    rows = row_tiles * halves
    pack(out_ref, forward(tiles_ref, slots_ref, primal_out, row_tiles, col_tiles))
    out_ref[rows : rows + 8, :] = jnp.broadcast_to(square_sum(change * change), (8, LANES))
    if iteration == 0:
        pack(out_ref, forward(tiles_ref, slots_ref, primal_ref, row_tiles, col_tiles), rows + 8)


def dual_kernel(*refs, last, first, part_count, col_tiles):
    refs = list(refs)
    part_refs = refs[:part_count]
    refs = refs[part_count:]
    scalars_ref, step_ref, dual_ref, side_ref, kind_ref = refs[:5]
    refs = refs[5:]
    if not first:
        image_ref = refs.pop(0)
    if not last:
        slots_ref, tiles_ref = refs[:2]
        refs = refs[2:]
    dual_out = refs.pop(0)

    values = [ref[...] for ref in part_refs]
    while len(values) > 1:
        values = [values[i] + values[i + 1] for i in range(0, len(values), 2)]
    total = values[0]
    row_tiles, width = dual_ref.shape
    weight = scalars_ref[0:1, 0:1]
    rows = row_tiles * (width // LANES)
    image_next = unpack(total, row_tiles, width)
    image = unpack(total, row_tiles, width, rows + 8) if first else image_ref[...]
    dual = dual_ref[...]
    step_size = step_ref[0:1, 0:1]
    values = dual + (step_size * weight) * (side_ref[...] - 2.0 * image_next + image)
    dual_next = jnp.where(kind_ref[...] == 1, jnp.maximum(values, 0.0), values)
    dual_out[...] = dual_next
    if last:
        return
    out_ref, image_out, moved_out = refs[:3]
    image_out[...] = image_next
    moved_out[...] = total[rows : rows + 8]
    change = dual_next - dual
    cross = square_sum(change * (image_next - image))
    dual_square = square_sum(change * change)
    meta = tiles_ref.shape[0] * (width // LANES)
    which = lax.broadcasted_iota(jnp.int32, (8, LANES), 0)
    out_ref[meta : meta + 8, :] = jnp.where(
        which == 0, cross, jnp.where(which == 1, dual_square, 0.0)
    )
    backward(tiles_ref, slots_ref, dual_next, out_ref, col_tiles)


def call(kernel, outs, inputs, scratch=(), spaces=None):
    spaces = spaces or {}
    specs = [
        pl.BlockSpec(memory_space=spaces.get(i, pltpu.VMEM)) for i in range(len(inputs))
    ]
    return pl.pallas_call(
        kernel,
        out_shape=outs,
        in_specs=specs,
        out_specs=[pl.BlockSpec(memory_space=pltpu.VMEM) for _ in outs],
        scratch_shapes=scratch,
        compiler_params=pltpu.CompilerParams(vmem_limit_bytes=32 * 1024 * 1024),
    )(*inputs)


def exchange(values, axis, size):
    others = [
        lax.ppermute(values, axis, [(i, i ^ k) for i in range(size)]) for k in range(1, size)
    ]
    return [values] + others


def gather_rows(values, size):
    copies = jnp.broadcast_to(values[None], (size,) + values.shape)
    return lax.all_to_all(copies, "row", split_axis=0, concat_axis=0)


def shards(
    matrix_tiles,
    tile_slot,
    cost_vector,
    lower_bound,
    bound_width,
    variable_kind,
    right_side,
    row_kind,
    primal_start,
    dual_start,
    primal_weight,
    step_start,
):
    tile_set = matrix_tiles[0, 0]
    slots = tile_slot[0, 0]
    row_tiles, width = right_side.shape
    col_tiles = cost_vector.shape[0]
    tile_count = slots.shape[0]
    row_count = lax.axis_size("row")
    col_count = lax.axis_size("col")
    scalars = jnp.where(
        lax.broadcasted_iota(jnp.int32, (8, LANES), 0) == 0, primal_weight, step_start
    )
    smem = pltpu.SMEM
    halves = width // LANES

    def array(*shape):
        return jax.ShapeDtypeStruct(shape, jnp.float32)

    (sent,) = call(
        functools.partial(start_kernel, col_tiles=col_tiles),
        [array(tile_count * (halves + 1), LANES)],
        [slots, tile_set, dual_start],
        spaces={0: smem},
    )
    primal, dual = primal_start, dual_start
    hot = step_size = moved = image = None
    for iteration in range(ITERS):
        first, last = iteration == 0, iteration + 1 == ITERS
        arrived = gather_rows(sent, row_count)
        sources = row_count * tile_count
        rows = row_tiles * halves
        outs = [
            array(rows + 8 + (rows if first else 0), LANES),
            array(*primal.shape),
            array(8, LANES),
        ]
        inputs = [slots, scalars, arrived, tile_set, primal]
        inputs += [cost_vector, lower_bound, bound_width, variable_kind]
        if first:
            outs.append(array(sources, col_tiles))
        else:
            inputs += [hot, step_size, moved]
        results = call(
            functools.partial(primal_kernel, iteration=iteration, row_tiles=row_tiles),
            outs,
            inputs,
            scratch=[pltpu.VMEM((sources, width), jnp.float32)],
            spaces={0: smem},
        )
        image_part, primal, step_size = results[:3]
        if first:
            hot = results[3]
        parts = exchange(image_part, "col", col_count)
        outs = [array(*dual.shape)]
        inputs = [*parts, scalars, step_size, dual, right_side, row_kind]
        spaces = {}
        if not first:
            inputs.append(image)
        if not last:
            spaces[len(inputs)] = smem
            inputs += [slots, tile_set]
            outs += [array(tile_count * halves + 8, LANES), array(*dual.shape), array(8, LANES)]
        results = call(
            functools.partial(
                dual_kernel, last=last, first=first, part_count=len(parts), col_tiles=col_tiles
            ),
            outs,
            inputs,
            spaces=spaces,
        )
        dual = results[0]
        if not last:
            sent, image, moved = results[1:]
    return (primal, dual)


def solution(mesh):
    return jax.shard_map(
        shards,
        mesh=mesh,
        in_specs=(
            P("row", "col", None, None, None),
            P("row", "col", None),
            P("col", None),
            P("col", None),
            P("col", None),
            P("col", None),
            P("row", None),
            P("row", None),
            P("col", None),
            P("row", None),
            P(),
            P(),
        ),
        out_specs=(P("col", None), P("row", None)),
        check_vma=False,
    )
```

```python
import functools

import jax
import jax.numpy as jnp
from jax import lax
from jax.experimental import pallas as pl
from jax.experimental.pallas import tpu as pltpu
from jax.sharding import PartitionSpec as P

ITERS = 4
LANES = 128

highest = lax.Precision.HIGHEST


def square_sum(values):
    return jnp.sum(jnp.sum(values, axis=0, keepdims=True), axis=1, keepdims=True)


def columns_of(rows):
    count, width = rows.shape
    padded = jnp.concatenate([rows, jnp.zeros((128 - count, width), rows.dtype)], axis=0)
    return padded.T


def forward(tiles_ref, slots_ref, vector_ref, row_tiles, col_tiles):
    tile_count, height, width = tiles_ref.shape
    lane = lax.broadcasted_iota(jnp.int32, (height, 128), 1)

    def step(t, total):
        slot = slots_ref[t]
        picked = vector_ref[pl.ds(slot % col_tiles, 1), :]
        product = jnp.sum(tiles_ref[t] * picked, axis=1, keepdims=True)
        return total + jnp.where(lane == slot // col_tiles, product, 0.0)

    total = lax.fori_loop(0, tile_count, step, jnp.zeros((height, 128), jnp.float32), unroll=2)
    return total.T[:row_tiles]


def backward(tiles_ref, slots_ref, rows, out_ref, col_tiles, ready=None):
    tile_count, height, width = tiles_ref.shape
    columns = columns_of(rows)
    lane = lax.broadcasted_iota(jnp.int32, columns.shape, 1)
    halves = width // LANES

    def step(t, carry):
        slot = slots_ref[t]
        if ready is not None:
            ready(t)
        mine = jnp.where(lane == slot // col_tiles, columns, 0.0)
        picked = jnp.sum(mine, axis=1, keepdims=True)
        product = jnp.sum(tiles_ref[t] * picked, axis=0, keepdims=True)
        for h in range(halves):
            out_ref[pl.ds(h * tile_count + t, 1), :] = product[:, h * LANES : (h + 1) * LANES]
        return carry

    lax.fori_loop(0, tile_count, step, 0, unroll=2)


def pack(out_ref, values, start=0):
    count, width = values.shape
    for h in range(width // LANES):
        block = values[:, h * LANES : (h + 1) * LANES]
        out_ref[start + h * count : start + (h + 1) * count, :] = block


def unpack(values, count, width, start=0):
    blocks = [
        values[start + h * count : start + (h + 1) * count] for h in range(width // LANES)
    ]
    return jnp.concatenate(blocks, axis=1)


def start_kernel(
    slots_hbm,
    tiles_hbm,
    dual_hbm,
    weight_ref,
    step_ref,
    out_ref,
    scalars_out,
    slots_ref,
    tiles_ref,
    dual_ref,
    sems,
    *,
    col_tiles,
):
    tile_count, height, width = tiles_ref.shape

    def tile_copy(t):
        return pltpu.make_async_copy(tiles_hbm.at[t], tiles_ref.at[t], sems.at[t])

    slots_copy = pltpu.make_async_copy(slots_hbm, slots_ref, sems.at[tile_count])
    dual_copy = pltpu.make_async_copy(dual_hbm, dual_ref, sems.at[tile_count + 1])
    slots_copy.start()
    dual_copy.start()
    for t in range(tile_count):
        tile_copy(t).start()
    which = lax.broadcasted_iota(jnp.int32, scalars_out.shape, 0)
    scalars_out[...] = jnp.where(which == 0, weight_ref[0], step_ref[0])
    slots_copy.wait()
    meta = tile_count * (width // LANES)
    for t in range(tile_count):
        column = slots_ref[t] % col_tiles
        out_ref[meta + t : meta + t + 1, :] = jnp.full((1, LANES), column, jnp.int32).astype(
            jnp.float32
        )
    dual_copy.wait()
    backward(
        tiles_ref,
        slots_ref,
        dual_ref[...],
        out_ref,
        col_tiles,
        ready=lambda t: tile_copy(t).wait(),
    )


def primal_kernel(*refs, iteration, row_tiles):
    slots_ref, scalars_ref, arrived_ref = refs[:3]
    tiles_ref, primal_ref, cost_ref, lower_ref, width_ref, kind_ref = refs[3:9]
    refs = refs[9:]
    if iteration > 0:
        hot_ref, step_ref, moved_ref = refs[:3]
        refs = refs[3:]
    out_ref, primal_out, step_out = refs[:3]
    refs = refs[3:]
    if iteration == 0:
        hot_ref = refs[0]
        refs = refs[1:]
    gather_ref = refs[0]

    col_tiles, width = primal_ref.shape
    tile_count = tiles_ref.shape[0]
    sources = arrived_ref.shape[0]
    halves = width // LANES
    meta = tile_count * halves
    for r in range(sources):
        for h in range(halves):
            gather_ref[r * tile_count : (r + 1) * tile_count, h * LANES : (h + 1) * LANES] = (
                arrived_ref[r, h * tile_count : (h + 1) * tile_count, :]
            )
    weight = scalars_ref[0:1, 0:1]
    if iteration == 0:
        number = lax.broadcasted_iota(jnp.int32, (tile_count, col_tiles), 1).astype(jnp.float32)
        for r in range(sources):
            column = arrived_ref[r, meta : meta + tile_count, :]
            hot_ref[r * tile_count : (r + 1) * tile_count, :] = (
                column[:, 0:1] == number
            ).astype(jnp.float32)
        step_size = scalars_ref[1:2, 0:1]
    else:
        sums = arrived_ref[0, meta : meta + 8, :]
        for r in range(1, sources):
            sums = sums + arrived_ref[r, meta : meta + 8, :]
        cross = sums[0:1, 0:1]
        dual_square = sums[1:2, 0:1]
        primal_square = moved_ref[0:1, 0:1]
        before = step_ref[0:1, 0:1]
        movement = 0.5 * weight * primal_square + 0.5 * dual_square / weight
        count = iteration - 1 + 11.0
        step_size = movement / jnp.maximum(
            jnp.abs(cross) / (1.0 - count ** (-0.3)),
            movement / ((1.0 + count ** (-0.6)) * before),
        )
    step_out[...] = jnp.broadcast_to(step_size, step_out.shape)
    gradient = lax.dot_general(
        hot_ref[...],
        gather_ref[...],
        (((0,), (0,)), ((), ())),
        precision=highest,
        preferred_element_type=jnp.float32,
    )
    primal = primal_ref[...]
    kind = kind_ref[...]
    lower = lower_ref[...]
    values = primal - (step_size / weight) * (cost_ref[...] - gradient)
    lifted = jnp.where(kind >= 1, jnp.maximum(values, lower), values)
    primal_next = jnp.where(kind == 2, jnp.minimum(lifted, lower + width_ref[...]), lifted)
    primal_out[...] = primal_next
    change = primal_next - primal
    rows = row_tiles * halves
    pack(out_ref, forward(tiles_ref, slots_ref, primal_out, row_tiles, col_tiles))
    out_ref[rows : rows + 8, :] = jnp.broadcast_to(square_sum(change * change), (8, LANES))
    if iteration == 0:
        pack(out_ref, forward(tiles_ref, slots_ref, primal_ref, row_tiles, col_tiles), rows + 8)


def dual_kernel(*refs, last, first, part_count, col_tiles):
    refs = list(refs)
    part_refs = refs[:part_count]
    refs = refs[part_count:]
    scalars_ref, step_ref, dual_ref, side_ref, kind_ref = refs[:5]
    refs = refs[5:]
    if not first:
        image_ref = refs.pop(0)
    if not last:
        slots_ref, tiles_ref = refs[:2]
        refs = refs[2:]
    dual_out = refs.pop(0)

    values = [ref[...] for ref in part_refs]
    while len(values) > 1:
        values = [values[i] + values[i + 1] for i in range(0, len(values), 2)]
    total = values[0]
    row_tiles, width = dual_ref.shape
    weight = scalars_ref[0:1, 0:1]
    rows = row_tiles * (width // LANES)
    image_next = unpack(total, row_tiles, width)
    image = unpack(total, row_tiles, width, rows + 8) if first else image_ref[...]
    dual = dual_ref[...]
    step_size = step_ref[0:1, 0:1]
    values = dual + (step_size * weight) * (side_ref[...] - 2.0 * image_next + image)
    dual_next = jnp.where(kind_ref[...] == 1, jnp.maximum(values, 0.0), values)
    dual_out[...] = dual_next
    if last:
        return
    out_ref, image_out, moved_out = refs[:3]
    image_out[...] = image_next
    moved_out[...] = total[rows : rows + 8]
    change = dual_next - dual
    cross = square_sum(change * (image_next - image))
    dual_square = square_sum(change * change)
    meta = tiles_ref.shape[0] * (width // LANES)
    which = lax.broadcasted_iota(jnp.int32, (8, LANES), 0)
    out_ref[meta : meta + 8, :] = jnp.where(
        which == 0, cross, jnp.where(which == 1, dual_square, 0.0)
    )
    backward(tiles_ref, slots_ref, dual_next, out_ref, col_tiles)


def call(kernel, outs, inputs, scratch=(), spaces=None):
    spaces = spaces or {}
    specs = [
        pl.BlockSpec(memory_space=spaces.get(i, pltpu.VMEM)) for i in range(len(inputs))
    ]
    return pl.pallas_call(
        kernel,
        out_shape=outs,
        in_specs=specs,
        out_specs=[pl.BlockSpec(memory_space=pltpu.VMEM) for _ in outs],
        scratch_shapes=scratch,
        compiler_params=pltpu.CompilerParams(vmem_limit_bytes=32 * 1024 * 1024),
    )(*inputs)


def exchange(values, axis, size):
    others = [
        lax.ppermute(values, axis, [(i, i ^ k) for i in range(size)]) for k in range(1, size)
    ]
    return [values] + others


def gather_rows(values, size):
    copies = jnp.broadcast_to(values[None], (size,) + values.shape)
    return lax.all_to_all(copies, "row", split_axis=0, concat_axis=0)


def shards(
    matrix_tiles,
    tile_slot,
    cost_vector,
    lower_bound,
    bound_width,
    variable_kind,
    right_side,
    row_kind,
    primal_start,
    dual_start,
    primal_weight,
    step_start,
):
    tile_set = matrix_tiles[0, 0]
    slots = tile_slot[0, 0]
    row_tiles, width = right_side.shape
    col_tiles = cost_vector.shape[0]
    tile_count = slots.shape[0]
    row_count = lax.axis_size("row")
    col_count = lax.axis_size("col")
    smem = pltpu.SMEM
    halves = width // LANES

    def array(*shape):
        return jax.ShapeDtypeStruct(shape, jnp.float32)

    sent, scalars = call(
        functools.partial(start_kernel, col_tiles=col_tiles),
        [array(tile_count * (halves + 1), LANES), array(8, LANES)],
        [
            pltpu.with_memory_space_constraint(slots, pltpu.HBM),
            pltpu.with_memory_space_constraint(tile_set, pltpu.HBM),
            pltpu.with_memory_space_constraint(dual_start, pltpu.HBM),
            primal_weight.reshape(1),
            step_start.reshape(1),
        ],
        scratch=[
            pltpu.SMEM(slots.shape, jnp.int32),
            pltpu.VMEM(tile_set.shape, jnp.float32),
            pltpu.VMEM(dual_start.shape, jnp.float32),
            pltpu.SemaphoreType.DMA((tile_count + 2,)),
        ],
        spaces={0: pltpu.HBM, 1: pltpu.HBM, 2: pltpu.HBM, 3: smem, 4: smem},
    )
    primal, dual = primal_start, dual_start
    hot = step_size = moved = image = None
    for iteration in range(ITERS):
        first, last = iteration == 0, iteration + 1 == ITERS
        arrived = gather_rows(sent, row_count)
        sources = row_count * tile_count
        rows = row_tiles * halves
        outs = [
            array(rows + 8 + (rows if first else 0), LANES),
            array(*primal.shape),
            array(8, LANES),
        ]
        inputs = [slots, scalars, arrived, tile_set, primal]
        inputs += [cost_vector, lower_bound, bound_width, variable_kind]
        if first:
            outs.append(array(sources, col_tiles))
        else:
            inputs += [hot, step_size, moved]
        results = call(
            functools.partial(primal_kernel, iteration=iteration, row_tiles=row_tiles),
            outs,
            inputs,
            scratch=[pltpu.VMEM((sources, width), jnp.float32)],
            spaces={0: smem},
        )
        image_part, primal, step_size = results[:3]
        if first:
            hot = results[3]
        parts = exchange(image_part, "col", col_count)
        outs = [array(*dual.shape)]
        inputs = [*parts, scalars, step_size, dual, right_side, row_kind]
        spaces = {}
        if not first:
            inputs.append(image)
        if not last:
            spaces[len(inputs)] = smem
            inputs += [slots, tile_set]
            outs += [array(tile_count * halves + 8, LANES), array(*dual.shape), array(8, LANES)]
        results = call(
            functools.partial(
                dual_kernel, last=last, first=first, part_count=len(parts), col_tiles=col_tiles
            ),
            outs,
            inputs,
            spaces=spaces,
        )
        dual = results[0]
        if not last:
            sent, image, moved = results[1:]
    return (primal, dual)


def solution(mesh):
    return jax.shard_map(
        shards,
        mesh=mesh,
        in_specs=(
            P("row", "col", None, None, None),
            P("row", "col", None),
            P("col", None),
            P("col", None),
            P("col", None),
            P("col", None),
            P("row", None),
            P("row", None),
            P("col", None),
            P("row", None),
            P(),
            P(),
        ),
        out_specs=(P("col", None), P("row", None)),
        check_vma=False,
    )
```

```python
import functools

import jax
import jax.numpy as jnp
from jax import lax
from jax.experimental import pallas as pl
from jax.experimental.pallas import tpu as pltpu
from jax.sharding import PartitionSpec as P

ITERS = 4
LANES = 128

highest = lax.Precision.HIGHEST


def square_sum(values):
    return jnp.sum(jnp.sum(values, axis=0, keepdims=True), axis=1, keepdims=True)


def columns_of(rows):
    count, width = rows.shape
    padded = jnp.concatenate([rows, jnp.zeros((128 - count, width), rows.dtype)], axis=0)
    return padded.T


def forward(tiles_ref, slots_ref, vector_ref, row_tiles, col_tiles):
    tile_count, height, width = tiles_ref.shape
    lane = lax.broadcasted_iota(jnp.int32, (height, 128), 1)

    def step(t, total):
        slot = slots_ref[t]
        picked = vector_ref[pl.ds(slot % col_tiles, 1), :]
        product = jnp.sum(tiles_ref[t] * picked, axis=1, keepdims=True)
        return total + jnp.where(lane == slot // col_tiles, product, 0.0)

    total = lax.fori_loop(0, tile_count, step, jnp.zeros((height, 128), jnp.float32), unroll=4)
    return total.T[:row_tiles]


def backward(tiles_ref, slots_ref, rows, out_ref, col_tiles, ready=None):
    tile_count, height, width = tiles_ref.shape
    columns = columns_of(rows)
    lane = lax.broadcasted_iota(jnp.int32, columns.shape, 1)
    halves = width // LANES

    def step(t, carry):
        slot = slots_ref[t]
        if ready is not None:
            ready(t)
        mine = jnp.where(lane == slot // col_tiles, columns, 0.0)
        picked = jnp.sum(mine, axis=1, keepdims=True)
        product = jnp.sum(tiles_ref[t] * picked, axis=0, keepdims=True)
        for h in range(halves):
            out_ref[pl.ds(h * tile_count + t, 1), :] = product[:, h * LANES : (h + 1) * LANES]
        return carry

    lax.fori_loop(0, tile_count, step, 0, unroll=4)


def pack(out_ref, values, start=0):
    count, width = values.shape
    for h in range(width // LANES):
        block = values[:, h * LANES : (h + 1) * LANES]
        out_ref[start + h * count : start + (h + 1) * count, :] = block


def unpack(values, count, width, start=0):
    blocks = [
        values[start + h * count : start + (h + 1) * count] for h in range(width // LANES)
    ]
    return jnp.concatenate(blocks, axis=1)


def start_kernel(
    slots_hbm,
    tiles_hbm,
    dual_hbm,
    weight_ref,
    step_ref,
    out_ref,
    scalars_out,
    slots_ref,
    tiles_ref,
    dual_ref,
    sems,
    *,
    col_tiles,
):
    tile_count, height, width = tiles_ref.shape

    def tile_copy(t):
        return pltpu.make_async_copy(tiles_hbm.at[t], tiles_ref.at[t], sems.at[t])

    slots_copy = pltpu.make_async_copy(slots_hbm, slots_ref, sems.at[tile_count])
    dual_copy = pltpu.make_async_copy(dual_hbm, dual_ref, sems.at[tile_count + 1])
    slots_copy.start()
    dual_copy.start()
    for t in range(tile_count):
        tile_copy(t).start()
    which = lax.broadcasted_iota(jnp.int32, scalars_out.shape, 0)
    scalars_out[...] = jnp.where(which == 0, weight_ref[0], step_ref[0])
    slots_copy.wait()
    meta = tile_count * (width // LANES)
    for t in range(tile_count):
        column = slots_ref[t] % col_tiles
        out_ref[meta + t : meta + t + 1, :] = jnp.full((1, LANES), column, jnp.int32).astype(
            jnp.float32
        )
    dual_copy.wait()
    backward(
        tiles_ref,
        slots_ref,
        dual_ref[...],
        out_ref,
        col_tiles,
        ready=lambda t: tile_copy(t).wait(),
    )


def primal_kernel(*refs, iteration, row_tiles):
    slots_ref, scalars_ref, arrived_ref = refs[:3]
    tiles_ref, primal_ref, cost_ref, lower_ref, width_ref, kind_ref = refs[3:9]
    refs = refs[9:]
    if iteration > 0:
        hot_ref, step_ref, moved_ref = refs[:3]
        refs = refs[3:]
    out_ref, primal_out, step_out = refs[:3]
    refs = refs[3:]
    if iteration == 0:
        hot_ref = refs[0]
        refs = refs[1:]
    gather_ref = refs[0]

    col_tiles, width = primal_ref.shape
    tile_count = tiles_ref.shape[0]
    sources = arrived_ref.shape[0]
    halves = width // LANES
    meta = tile_count * halves
    for r in range(sources):
        for h in range(halves):
            gather_ref[r * tile_count : (r + 1) * tile_count, h * LANES : (h + 1) * LANES] = (
                arrived_ref[r, h * tile_count : (h + 1) * tile_count, :]
            )
    weight = scalars_ref[0:1, 0:1]
    if iteration == 0:
        number = lax.broadcasted_iota(jnp.int32, (tile_count, col_tiles), 1).astype(jnp.float32)
        for r in range(sources):
            column = arrived_ref[r, meta : meta + tile_count, :]
            hot_ref[r * tile_count : (r + 1) * tile_count, :] = (
                column[:, 0:1] == number
            ).astype(jnp.float32)
        step_size = scalars_ref[1:2, 0:1]
    else:
        sums = arrived_ref[0, meta : meta + 8, :]
        for r in range(1, sources):
            sums = sums + arrived_ref[r, meta : meta + 8, :]
        cross = sums[0:1, 0:1]
        dual_square = sums[1:2, 0:1]
        primal_square = moved_ref[0:1, 0:1]
        before = step_ref[0:1, 0:1]
        movement = 0.5 * weight * primal_square + 0.5 * dual_square / weight
        count = iteration - 1 + 11.0
        step_size = movement / jnp.maximum(
            jnp.abs(cross) / (1.0 - count ** (-0.3)),
            movement / ((1.0 + count ** (-0.6)) * before),
        )
    step_out[...] = jnp.broadcast_to(step_size, step_out.shape)
    gradient = lax.dot_general(
        hot_ref[...],
        gather_ref[...],
        (((0,), (0,)), ((), ())),
        precision=highest,
        preferred_element_type=jnp.float32,
    )
    primal = primal_ref[...]
    kind = kind_ref[...]
    lower = lower_ref[...]
    values = primal - (step_size / weight) * (cost_ref[...] - gradient)
    lifted = jnp.where(kind >= 1, jnp.maximum(values, lower), values)
    primal_next = jnp.where(kind == 2, jnp.minimum(lifted, lower + width_ref[...]), lifted)
    primal_out[...] = primal_next
    change = primal_next - primal
    rows = row_tiles * halves
    pack(out_ref, forward(tiles_ref, slots_ref, primal_out, row_tiles, col_tiles))
    out_ref[rows : rows + 8, :] = jnp.broadcast_to(square_sum(change * change), (8, LANES))
    if iteration == 0:
        pack(out_ref, forward(tiles_ref, slots_ref, primal_ref, row_tiles, col_tiles), rows + 8)


def dual_kernel(*refs, last, first, part_count, col_tiles):
    refs = list(refs)
    part_refs = refs[:part_count]
    refs = refs[part_count:]
    scalars_ref, step_ref, dual_ref, side_ref, kind_ref = refs[:5]
    refs = refs[5:]
    if not first:
        image_ref = refs.pop(0)
    if not last:
        slots_ref, tiles_ref = refs[:2]
        refs = refs[2:]
    dual_out = refs.pop(0)

    values = [ref[...] for ref in part_refs]
    while len(values) > 1:
        values = [values[i] + values[i + 1] for i in range(0, len(values), 2)]
    total = values[0]
    row_tiles, width = dual_ref.shape
    weight = scalars_ref[0:1, 0:1]
    rows = row_tiles * (width // LANES)
    image_next = unpack(total, row_tiles, width)
    image = unpack(total, row_tiles, width, rows + 8) if first else image_ref[...]
    dual = dual_ref[...]
    step_size = step_ref[0:1, 0:1]
    values = dual + (step_size * weight) * (side_ref[...] - 2.0 * image_next + image)
    dual_next = jnp.where(kind_ref[...] == 1, jnp.maximum(values, 0.0), values)
    dual_out[...] = dual_next
    if last:
        return
    out_ref, image_out, moved_out = refs[:3]
    image_out[...] = image_next
    moved_out[...] = total[rows : rows + 8]
    change = dual_next - dual
    cross = square_sum(change * (image_next - image))
    dual_square = square_sum(change * change)
    meta = tiles_ref.shape[0] * (width // LANES)
    which = lax.broadcasted_iota(jnp.int32, (8, LANES), 0)
    out_ref[meta : meta + 8, :] = jnp.where(
        which == 0, cross, jnp.where(which == 1, dual_square, 0.0)
    )
    backward(tiles_ref, slots_ref, dual_next, out_ref, col_tiles)


def call(kernel, outs, inputs, scratch=(), spaces=None):
    spaces = spaces or {}
    specs = [
        pl.BlockSpec(memory_space=spaces.get(i, pltpu.VMEM)) for i in range(len(inputs))
    ]
    return pl.pallas_call(
        kernel,
        out_shape=outs,
        in_specs=specs,
        out_specs=[pl.BlockSpec(memory_space=pltpu.VMEM) for _ in outs],
        scratch_shapes=scratch,
        compiler_params=pltpu.CompilerParams(vmem_limit_bytes=32 * 1024 * 1024),
    )(*inputs)


def exchange(values, axis, size):
    others = [
        lax.ppermute(values, axis, [(i, i ^ k) for i in range(size)]) for k in range(1, size)
    ]
    return [values] + others


def gather_rows(values, size):
    copies = jnp.broadcast_to(values[None], (size,) + values.shape)
    return lax.all_to_all(copies, "row", split_axis=0, concat_axis=0)


def shards(
    matrix_tiles,
    tile_slot,
    cost_vector,
    lower_bound,
    bound_width,
    variable_kind,
    right_side,
    row_kind,
    primal_start,
    dual_start,
    primal_weight,
    step_start,
):
    tile_set = matrix_tiles[0, 0]
    slots = tile_slot[0, 0]
    row_tiles, width = right_side.shape
    col_tiles = cost_vector.shape[0]
    tile_count = slots.shape[0]
    row_count = lax.axis_size("row")
    col_count = lax.axis_size("col")
    smem = pltpu.SMEM
    halves = width // LANES

    def array(*shape):
        return jax.ShapeDtypeStruct(shape, jnp.float32)

    sent, scalars = call(
        functools.partial(start_kernel, col_tiles=col_tiles),
        [array(tile_count * (halves + 1), LANES), array(8, LANES)],
        [
            pltpu.with_memory_space_constraint(slots, pltpu.HBM),
            pltpu.with_memory_space_constraint(tile_set, pltpu.HBM),
            pltpu.with_memory_space_constraint(dual_start, pltpu.HBM),
            primal_weight.reshape(1),
            step_start.reshape(1),
        ],
        scratch=[
            pltpu.SMEM(slots.shape, jnp.int32),
            pltpu.VMEM(tile_set.shape, jnp.float32),
            pltpu.VMEM(dual_start.shape, jnp.float32),
            pltpu.SemaphoreType.DMA((tile_count + 2,)),
        ],
        spaces={0: pltpu.HBM, 1: pltpu.HBM, 2: pltpu.HBM, 3: smem, 4: smem},
    )
    primal, dual = primal_start, dual_start
    hot = step_size = moved = image = None
    for iteration in range(ITERS):
        first, last = iteration == 0, iteration + 1 == ITERS
        arrived = gather_rows(sent, row_count)
        sources = row_count * tile_count
        rows = row_tiles * halves
        outs = [
            array(rows + 8 + (rows if first else 0), LANES),
            array(*primal.shape),
            array(8, LANES),
        ]
        inputs = [slots, scalars, arrived, tile_set, primal]
        inputs += [cost_vector, lower_bound, bound_width, variable_kind]
        if first:
            outs.append(array(sources, col_tiles))
        else:
            inputs += [hot, step_size, moved]
        results = call(
            functools.partial(primal_kernel, iteration=iteration, row_tiles=row_tiles),
            outs,
            inputs,
            scratch=[pltpu.VMEM((sources, width), jnp.float32)],
            spaces={0: smem},
        )
        image_part, primal, step_size = results[:3]
        if first:
            hot = results[3]
        parts = exchange(image_part, "col", col_count)
        outs = [array(*dual.shape)]
        inputs = [*parts, scalars, step_size, dual, right_side, row_kind]
        spaces = {}
        if not first:
            inputs.append(image)
        if not last:
            spaces[len(inputs)] = smem
            inputs += [slots, tile_set]
            outs += [array(tile_count * halves + 8, LANES), array(*dual.shape), array(8, LANES)]
        results = call(
            functools.partial(
                dual_kernel, last=last, first=first, part_count=len(parts), col_tiles=col_tiles
            ),
            outs,
            inputs,
            spaces=spaces,
        )
        dual = results[0]
        if not last:
            sent, image, moved = results[1:]
    return (primal, dual)


def solution(mesh):
    return jax.shard_map(
        shards,
        mesh=mesh,
        in_specs=(
            P("row", "col", None, None, None),
            P("row", "col", None),
            P("col", None),
            P("col", None),
            P("col", None),
            P("col", None),
            P("row", None),
            P("row", None),
            P("col", None),
            P("row", None),
            P(),
            P(),
        ),
        out_specs=(P("col", None), P("row", None)),
        check_vma=False,
    )
```
